128 devices in a mesh: wide: 2 (over core), op: 64 (over z, y, x).
Axes of the slice: x: 4, y: 4, z: 4, core: 2. Of those that a mesh axis runs over, the one named last changes fastest.
Arguments:
- wavefunction: bfloat16 [32, 4, 512, 512], P('wide', None, 'op'), may hold values from -6 to 6
- left_ops: bfloat16 [512, 512, 512], P(('wide', 'op')), may hold values from -0.01953125 to 0.01953125
- right_ops: bfloat16 [512, 512, 512], P(('wide', 'op')), may hold values from -0.25 to 0.25
- in_sector: int32 [512], P(('wide', 'op')), may hold values from 0 to 31
- live_count: int32 [128], P(('wide', 'op')), may hold values from 2 to 4, as said below
Outputs:
- sigma_blocks: bfloat16 [2, 4, 512, 512], P('wide', None, 'op')
The draws below stay inside these ranges and needn't reach their ends.
Inputs may be any that keep to these rules, and one draw needn't show every extreme that they name: `live_count`: in each aligned group of 64 entries (the devices of one op group), entries i and i + 32 sum to 6, and exactly 16 entries are 4.
All inputs are finite; a program needn't handle non-finite values.
Results may differ from the reference program's by a relative error of at most 0.0065.
Values may be sent and summed in bfloat16 or wider, within the bound.
No kernel may reach another device: no remote copies, remote signals or barrier semaphores. Data moves between devices by JAX's collectives and lax.ppermute only.
A program may use at most 64 MiB of HBM per device.

```python
import jax
import jax.numpy as jnp
from jax import lax

M = 512
S = 4
SLOTS = 4
SECT = 32
TASKS = 512
N_WIDE = 2
N_OP = 64


def draw_live_count(key, part):
    half_size = N_OP // 2
    heavy_count = N_OP // 4
    subkeys = jax.random.split(jax.random.fold_in(key, 7), N_WIDE)

    def one_group(subkey):
        order_key, side_key = jax.random.split(subkey)
        ranked = jax.random.permutation(order_key, jnp.arange(half_size, dtype=jnp.int32))
        side = jax.random.randint(side_key, (half_size,), 0, 2).astype(jnp.int32)
        first = jnp.where(ranked < heavy_count, jnp.where(side == 1, 4, 2), 3).astype(jnp.int32)
        second = (6 - first).astype(jnp.int32)
        return jnp.concatenate([first, second])
    return jax.vmap(one_group)(subkeys).reshape(-1).astype(jnp.int32)


def with_ends(drawn, stream_key, smallest, high):
    extent = drawn.shape
    place = [jax.random.randint(jax.random.fold_in(stream_key, axis), (), 0, extent[axis]) for axis in range(len(extent))]
    drawn = drawn.at[tuple(place)].set(smallest)
    longest = extent.index(max(extent))
    place[longest] = (place[longest] + 1) % extent[longest]
    return drawn.at[tuple(place)].set(high)


def block_levels(stream_key, dims, pieces, smallest, top_value):
    def one(axis_at, blocks):
        draws = jax.random.uniform(jax.random.fold_in(jax.random.fold_in(stream_key, 6), axis_at), (blocks,), jnp.float32, smallest / len(pieces), top_value / len(pieces))
        return jnp.repeat(jnp.exp(draws), dims[axis_at] // blocks).reshape((-1,) + (1,) * (len(dims) - axis_at - 1))

    loudness = one(*pieces[0])
    for cut in pieces[1:]:
        loudness = loudness * one(*cut)
    return loudness


def centred(stream_key, dims, deviation, bound, cuts=(), kind=jnp.bfloat16):
    entries = deviation * jax.random.normal(stream_key, dims, jnp.float32)
    if cuts:
        entries = entries * block_levels(stream_key, dims, cuts, -0.22, 0.18)
    return jnp.clip(entries, -bound, bound).astype(kind)


def setup_inputs(seed: int = 0) -> dict:
    arg_keys = jax.random.split(jax.random.key(seed), 6)
    wavefunction = centred(arg_keys[0], (SECT, S, M, M), 1.0, 6.0, ((0, 2), (2, 64)))
    left_ops = centred(arg_keys[1], (TASKS, M, M), (3 * M * N_OP) ** -0.5, 0.01953125, ((0, 128),))
    right_ops = centred(arg_keys[2], (TASKS, M, M), M ** -0.5, 0.25, ((0, 128),))
    in_sector = with_ends(jax.random.randint(arg_keys[3], (TASKS,), 0, SECT), jax.random.fold_in(arg_keys[3], 1), 0, SECT - 1).astype(jnp.int32)
    live_count = draw_live_count(jax.random.fold_in(arg_keys[5], 71), 0)
    return dict(wavefunction=wavefunction, left_ops=left_ops, right_ops=right_ops, in_sector=in_sector, live_count=live_count)


def sandwich(sector, left_op, right_op):
    half_step = jnp.einsum("smk,nk->smn", sector.astype(jnp.float32), right_op.astype(jnp.float32))
    half_step = lax.optimization_barrier(half_step.astype(jnp.bfloat16)).astype(jnp.float32)
    return jnp.einsum("im,smn->sin", left_op.astype(jnp.float32), half_step)


def reference(wavefunction, left_ops, right_ops, in_sector, live_count):
    slot_count = SLOTS
    device_total = live_count.shape[0]

    def visit(sigma_acc, device_id):
        partial_value = jnp.zeros(wavefunction.shape[1:], jnp.float32)
        for slot_index in range(slot_count):
            task_id = (device_id * slot_count + slot_index).astype(jnp.int32)
            sector = lax.dynamic_index_in_dim(wavefunction, in_sector[task_id].astype(jnp.int32), 0, keepdims=False)
            left_op = lax.dynamic_index_in_dim(left_ops, task_id, 0, keepdims=False)
            right_op = lax.dynamic_index_in_dim(right_ops, task_id, 0, keepdims=False)
            weight = (slot_index < live_count[device_id]).astype(jnp.float32)
            partial_value = partial_value + weight * sandwich(sector, left_op, right_op)
        owner = (device_id // N_OP).astype(jnp.int32)
        current = lax.dynamic_index_in_dim(sigma_acc, owner, 0, keepdims=False)
        sigma_acc = lax.dynamic_update_index_in_dim(sigma_acc, current + partial_value, owner, 0)
        return sigma_acc, None

    sigma_acc = jnp.zeros((N_WIDE,) + wavefunction.shape[1:], jnp.float32)
    sigma_acc, unused = lax.scan(visit, sigma_acc, jnp.arange(device_total, dtype=jnp.int32))
    return sigma_acc.astype(jnp.bfloat16)
```

```python
import functools

import jax
import jax.numpy as jnp
from jax import lax
from jax.experimental import pallas as pl
from jax.experimental.pallas import tpu as pltpu
from jax.sharding import Mesh, PartitionSpec as P

PLANE = ("y", "x")
CHUNKS = ((0, 2), (2, 3), (3, 4))


def from_behind(x, axis, by):
    n = lax.axis_size(axis)
    return lax.ppermute(x, axis, [(i, (i + by) % n) for i in range(n)])


def on_plane(x):
    return lax.all_to_all(x, PLANE, split_axis=0, concat_axis=0, tiled=True)


def pick_kernel(where_ref, own_ref, other_ref, out_ref):
    dests, slots = out_ref.shape[:2]
    half = own_ref.shape[0]
    mine = where_ref[0]
    first = pl.program_id(0) * dests

    def one(i, carry):
        dest, slot = i // slots, i % slots
        sector = where_ref[1 + (first + dest) * slots + slot]
        row = sector % half

        @pl.when(sector // half == mine)
        def _():
            out_ref[dest, slot] = own_ref[row]

        @pl.when(sector // half != mine)
        def _():
            out_ref[dest, slot] = other_ref[row]

        return carry

    lax.fori_loop(0, dests * slots, one, 0)


def picked(where, own, other, group, slots):
    block = own.shape[1:]
    dests = 4
    zeros = (0,) * len(block)
    return pl.pallas_call(
        pick_kernel,
        grid_spec=pltpu.PrefetchScalarGridSpec(
            num_scalar_prefetch=1,
            grid=(group // dests,),
            in_specs=[pl.BlockSpec(own.shape, lambda i, w: (0, *zeros))] * 2,
            out_specs=pl.BlockSpec((dests, slots, *block), lambda i, w: (i, 0, *zeros)),
        ),
        out_shape=jax.ShapeDtypeStruct((group, slots, *block), own.dtype),
        cost_estimate=pl.CostEstimate(
            flops=2 * own.size * 64, bytes_accessed=6 * own.size, transcendentals=0
        ),
        name="pick",
    )(where, own, other)


def sandwich_kernel(place_ref, psi_ref, left_ref, right_ref, left3_ref, right3_ref, *rest):
    outs, half_ref, total_ref = rest[:4], rest[4], rest[5]
    group, slots, states, rows, width = psi_ref.shape
    lines = len(outs)
    depth = rows // lines
    block = group * depth
    me = place_ref[0]
    for state in range(states):
        for slot in range(slots):
            left = left_ref[slot] if slot < 2 else left3_ref[...]
            right = right_ref[slot] if slot < 2 else right3_ref[...]
            psi = psi_ref[:, slot, state].reshape(group * rows, width)
            half = lax.dot_general(
                psi, right, (((1,), (1,)), ((), ())), preferred_element_type=jnp.float32
            )
            half = half.reshape(group, lines, depth, half.shape[-1])
            for k in range(lines):
                at = pl.multiple_of(((me + lines - k) % lines) * block, block)
                part = half[:, k].reshape(block, half.shape[-1])
                half_ref[pl.ds(at, block), :] = part.astype(half_ref.dtype)
            term = jnp.dot(left, half_ref[...], preferred_element_type=jnp.float32)
            if slot == 0:
                total_ref[...] = term
            else:
                total_ref[...] += term
        for k in range(lines):
            at = pl.multiple_of(((me + k) % lines) * block, block)
            outs[k][state] = total_ref[pl.ds(at, block), :].astype(outs[k].dtype)


def sandwiched(place, psi, left, right, left3, right3, lines):
    group, slots, states, rows, width = psi.shape
    size = left.shape[1]
    out = jax.ShapeDtypeStruct((states, size // lines, size), jnp.bfloat16)
    pair = pl.BlockSpec((2, size, size), lambda i, p: (0, 0, 0))
    single = pl.BlockSpec((size, size), lambda i, p: (0, 0))
    return pl.pallas_call(
        sandwich_kernel,
        grid_spec=pltpu.PrefetchScalarGridSpec(
            num_scalar_prefetch=1,
            grid=(states,),
            in_specs=[
                pl.BlockSpec((group, slots, 1, rows, width), lambda i, p: (0, 0, i, 0, 0)),
                pair,
                pair,
                single,
                single,
            ],
            out_specs=[pl.BlockSpec((1, size // lines, size), lambda i, p: (i, 0, 0))] * lines,
            scratch_shapes=[
                pltpu.VMEM((size, size), jnp.bfloat16),
                pltpu.VMEM((size, size), jnp.float32),
            ],
        ),
        out_shape=[out] * lines,
        cost_estimate=pl.CostEstimate(
            flops=4 * states * slots * size**3,
            bytes_accessed=2 * (psi.size + 6 * size * size + states * size * size),
            transcendentals=0,
        ),
        name="sandwich",
    )(place, psi, left, right, left3, right3)


def local(wavefunction, left_ops, right_ops, in_sector, live_count):
    lines = lax.axis_size("z")
    group = lax.axis_size("y") * lax.axis_size("x")
    own_third = live_count[0] >= 3
    place = lax.axis_index("z").astype(jnp.int32).reshape(1)
    wide = lax.axis_index("wide").astype(jnp.int32).reshape(1)

    surplus = from_behind(in_sector, "z", lines // 2)
    third = jnp.where(own_third, in_sector[2:3], surplus[3:4])
    work = jnp.concatenate([in_sector[:2], third])
    slots = work.shape[0]
    plane_work = on_plane(jnp.broadcast_to(work[None], (group, slots)))
    where = jnp.concatenate([wide, plane_work.reshape(-1)])

    arrived_left, arrived_right = (
        from_behind(ops[3], "z", lines // 2) for ops in (left_ops, right_ops)
    )
    left3 = jnp.where(own_third, left_ops[2], arrived_left)
    right3 = jnp.where(own_third, right_ops[2], arrived_right)

    rows = []
    for start, stop in CHUNKS:
        mine = wavefunction[:, start:stop]
        pieces = [mine] + [from_behind(mine, "z", k) for k in range(1, lines)]
        own = jnp.concatenate(pieces, axis=2)
        rows.append((own, from_behind(own, "wide", 1)))

    summed = []
    for own, other in rows:
        arrived = on_plane(picked(where, own, other, group, slots))
        blocks = sandwiched(place, arrived, left_ops, right_ops, left3, right3, lines)
        total = blocks[0].astype(jnp.float32)
        for k in range(1, lines):
            total = total + from_behind(blocks[k], "z", k).astype(jnp.float32)
        states, height, width = total.shape
        total = total.astype(jnp.bfloat16).reshape(states, group, height // group, width)
        summed.append(jnp.moveaxis(total, 1, 0))
    parts = on_plane(jnp.concatenate(summed, axis=1))
    return jnp.sum(parts.astype(jnp.float32), axis=0, keepdims=True).astype(jnp.bfloat16)


def solution(mesh):
    torus = Mesh(mesh.devices.reshape(2, 4, 4, 4), ("wide", "z", "y", "x"))
    op = ("z", "y", "x")
    each = ("wide", *op)
    placed = (P("wide", None, op, None), P(each, None, None), P(each, None, None), P(each), P(each))
    return jax.shard_map(
        local, mesh=torus, in_specs=placed, out_specs=P("wide", None, op, None), check_vma=False
    )
```
